32 devices in a mesh: groups: 2 (over x), dom: 16 (over z, y, core).
Axes of the slice: x: 2, y: 2, z: 4, core: 2. Of those that a mesh axis runs over, the one named last changes fastest.
Arguments:
- particles: bfloat16 [1024, 4096], P(('groups', 'dom')), parts along dimension 0, may hold values from -5 to 5
- dataset: bfloat16 [2048, 4096], P(('groups', 'dom')), parts along dimension 0, may hold values from -0.09375 to 0.09375
- labels: int32 [2048], P(('groups', 'dom')), parts along dimension 0, may hold values 0 or 1
- batch_index: int32 [512], P(('groups', 'dom')), parts along dimension 0, may hold values from 0 to 1023, as said below
Outputs:
- driving: float32 [1024, 4096], P(('groups', 'dom')), parts along dimension 0
- spreading: float32 [1024, 4096], P(('groups', 'dom')), parts along dimension 0
The draws below stay inside these ranges and needn't reach their ends.
There are 2 independent parts, one for each index of `groups`. The reference program is written for one: setup_inputs(seed, part) draws one part's arguments, and reference() takes and returns one part's arrays. A program takes and returns all parts, laid end to end along the dimension named above; each array names one. Nothing has to cross between parts.
Inputs may be any that keep to these rules, and one draw needn't show every extreme that they name: `batch_index`: entry b names a row of block b // 16 of the dataset, that is a row from (b // 16) * 64 to (b // 16 + 1) * 64 - 1; rows may repeat.
All inputs are finite; a program needn't handle non-finite values. No bound on the sum of `labels` on one device may be relied on, other than what follows from the above.
Results may differ from the reference program's by a relative error of at most 0.0003.
Values may be sent and summed in bfloat16 or wider, within the bound.
A program may use at most 128 MiB of HBM per device.

```python
import jax
import jax.numpy as jnp
from jax import lax

D = 4096
BATCH_DEV = 16
DATA_DEV = 64
NP = 512
BATCH = 256
DATA = 1024


def draw_particles(key, part):
    key_centre = jax.random.fold_in(key, 11)
    key_radius = jax.random.fold_in(key, 12)
    key_noise = jax.random.fold_in(key, 13)
    key_directions = jax.random.fold_in(key, 14)
    key_latent = jax.random.fold_in(key, 15)
    centre = 0.5 * jnp.clip(jax.random.normal(key_centre, (D,), jnp.float32), -4.0, 4.0)
    radii = jnp.exp(jax.random.uniform(key_radius, (NP, 1), jnp.float32, jnp.log(0.1), jnp.log(0.3)))
    directions = jax.random.normal(key_directions, (8, D), jnp.float32) / jnp.sqrt(jnp.float32(D))
    spread = jnp.sqrt(jnp.float32(0.0390625 * D))
    noise = jnp.clip(jax.random.normal(key_noise, (NP, D), jnp.float32), -4.0, 4.0)
    latent = spread * jnp.clip(jax.random.normal(key_latent, (NP, 8), jnp.float32), -4.0, 4.0)
    placed = jnp.dot(latent, directions)
    field = centre[None, :] + placed + radii * noise
    return jnp.clip(field, -5.0, 5.0).astype(jnp.bfloat16)


def draw_batch_index(key, part):
    block = jnp.arange(BATCH, dtype=jnp.int32) // BATCH_DEV
    offset = jax.random.randint(jax.random.fold_in(key, 21), (BATCH,), 0, DATA_DEV, jnp.int32)
    return (block * DATA_DEV + offset).astype(jnp.int32)


def place_ends(drawn, stream_key, least, top_value):
    longest = drawn.shape.index(max(drawn.shape))
    spots = []
    for shift in (0, 1):
        where = [jax.random.randint(jax.random.fold_in(stream_key, axis), (), 0, length) for axis, length in enumerate(drawn.shape)]
        where[longest] = (where[longest] + shift) % drawn.shape[longest]
        spots.append(tuple(where))
    return drawn.at[spots[0]].set(least).at[spots[1]].set(top_value)


def level_of(stream_key, shape, cuts, low, top_value):
    level, own = 1.0, jax.random.fold_in(stream_key, 6)
    for dim, parts in cuts:
        steps = jnp.exp(jax.random.uniform(jax.random.fold_in(own, dim), (parts,), jnp.float32, low / len(cuts), top_value / len(cuts)))
        level = level * jnp.repeat(steps, shape[dim] // parts).reshape([-1 if axis == dim else 1 for axis in range(len(shape))])
    return level


def normal_values(stream_key, extent, width, bound, cuts=(), held_as=jnp.bfloat16):
    level = level_of(stream_key, extent, cuts, -0.22, 0.18) if cuts else 1.0
    array = jax.random.normal(stream_key, extent, jnp.float32) * width * level
    return jnp.minimum(jnp.maximum(array, -bound), bound).astype(held_as)


def setup_inputs(seed: int = 0, part: int = 0) -> dict:
    key_list = jax.random.split(jax.random.key(seed), 5)
    part_splits = jax.random.split(jax.random.fold_in(key_list[4], part), 5)
    return {
        "particles": draw_particles(jax.random.fold_in(jax.random.fold_in(key_list[4], part), 71), part),
        "dataset": normal_values(part_splits[1], (DATA, D), D ** -0.5, 0.09375, ((0, 16),)),
        "labels": place_ends((jax.random.randint(part_splits[2], (DATA,), 0, 2) < 1).astype(jnp.int32), jax.random.fold_in(part_splits[2], 1), 0, 1),
        "batch_index": draw_batch_index(jax.random.fold_in(jax.random.fold_in(key_list[4], part), 71), part),
    }


prior_precision = 1.0


def reference(particles, dataset, labels, batch_index):
    rows = jnp.take(dataset, batch_index, axis=0)
    targets = jnp.take(labels, batch_index).astype(jnp.float32)
    particles_f = particles.astype(jnp.float32)
    logits = lax.dot_general(particles, rows, (((1,), (1,)), ((), ())), preferred_element_type=jnp.float32)
    misfit = (targets[None, :] - jax.nn.sigmoid(logits)).astype(jnp.bfloat16)
    pulled = jnp.dot(misfit, rows, preferred_element_type=jnp.float32)
    scores = (-prior_precision * particles_f + (DATA / BATCH) * pulled).astype(jnp.bfloat16)
    squares = jnp.sum(particles_f * particles_f, axis=1)
    cross = lax.dot_general(particles, particles, (((1,), (1,)), ((), ())), preferred_element_type=jnp.float32)
    dist = squares[:, None] + squares[None, :] - 2.0 * cross
    kernel_scale = 0.25 * D
    kernel = jnp.exp(-dist / kernel_scale)
    kernel_b = kernel.astype(jnp.bfloat16)
    rowsum = jnp.sum(kernel, axis=1)
    drive = jnp.dot(kernel_b, scores, preferred_element_type=jnp.float32)
    pull = jnp.dot(kernel_b, particles, preferred_element_type=jnp.float32)
    driving = drive / NP
    spreading = (particles_f * rowsum[:, None] - pull) / NP
    return driving, spreading
```

```python
import functools

import jax
import jax.numpy as jnp
from jax import lax
from jax.experimental import pallas as pl
from jax.experimental.pallas import tpu as pltpu
from jax.sharding import PartitionSpec as P

prior_precision = 1.0
MESH = pl.DeviceIdType.MESH
CROSS = 512
TILE = 512


class Stream:
    def __init__(self, buf, splits, recv, up, down, side, core):
        self.buf, self.splits, self.recv = buf, splits, recv
        self.sems = {"up": up, "down": down, "side": side, "core": core}


def kernel(n, particles, dataset, labels, index, drive_out, spread_out,
           held, rows, drive, pull, rowsum, target_row, own_sq, local_sem, *sems):
    planes = n // 4
    d = particles.shape[1]
    batch = rows.shape[0] * rows.shape[1]
    group = 4 * particles.shape[0]
    own_rows = dataset.shape[0]
    ratio = float(own_rows) / float(rows.shape[1])
    inv_scale = 1.0 / (0.25 * d)
    total = float(particles.shape[0] * n)

    me = lax.axis_index("dom")
    core = me % 2
    y = (me // 2) % 2
    z = me // 4
    target = {"up": me + 4, "down": me - 4, "side": me + 2 - 4 * y, "core": me + 1 - 2 * core}
    has_up, has_down = z < planes - 1, z > 0
    row_stream = Stream(rows, ((0, d - CROSS), (d - CROSS, CROSS + 128)), *sems[:5])
    part_stream = Stream(held, ((0, d - CROSS), (d - CROSS, CROSS)), *sems[5:])

    def block_of(p, yy, cc):
        return (p * 2 + yy) * 2 + cc

    def copy(st, k, b, way):
        view = st.buf.at[b, :, pl.ds(*st.splits[k])]
        return pltpu.make_async_remote_copy(
            src_ref=view, dst_ref=view, send_sem=st.sems[way].at[k, b], recv_sem=st.recv.at[k, b],
            device_id={"dom": target[way]}, device_id_type=MESH)

    def send(st, k, b, way, go):
        c = copy(st, k, b, way)
        c.start() if go else c.wait_send()

    def arrived(st, k, b):
        copy(st, k, b, "core").wait_recv()

    def own(st, go):
        for k in (1, 0):
            send(st, k, me, "side", go)

            @pl.when(has_up)
            def _():
                send(st, k, me, "up", go)

            @pl.when(has_down)
            def _():
                send(st, k, me, "down", go)

            send(st, k, me, "core", go)

    def own_cross(st, go):
        b = target["side"]
        if go:
            arrived(st, 1, b)

        @pl.when(has_up)
        def _():
            send(st, 1, b, "up", go)

        @pl.when(has_down)
        def _():
            send(st, 1, b, "down", go)

        send(st, 1, b, "core", go)

    def relay(st, p, go):
        for k, b, crosses in ((1, block_of(p, y, core), False), (0, block_of(p, y, core), True),
                              (1, block_of(p, 1 - y, core), False)):
            if go:
                arrived(st, k, b)

            @pl.when(jnp.logical_and(p > z, has_down))
            def _():
                send(st, k, b, "down", go)

            @pl.when(jnp.logical_and(p < z, has_up))
            def _():
                send(st, k, b, "up", go)

            if crosses:
                send(st, k, b, "side", go)
            send(st, k, b, "core", go)

    def finish_side(st, p, go):
        b = block_of(p, 1 - y, core)
        if go:
            arrived(st, 0, b)
        send(st, 0, b, "core", go)

    def finish_core(st, p):
        for yy in (0, 1):
            for k in (1, 0):
                arrived(st, k, block_of(p, yy, 1 - core))

    near = jnp.minimum(z, planes - 1 - z)
    outward = jnp.where(z <= planes - 1 - z, 1, -1)

    def distance(q):
        return jnp.where(q <= 2 * near, (q + 1) // 2, q - near)

    def plane(q):
        two_sided = jnp.where(q % 2 == 1, -1, 1)
        return z + jnp.where(q <= 2 * near, two_sided, outward) * distance(q)

    def within(s):
        return jnp.minimum(z, s) + jnp.minimum(planes - 1 - z, s) + 1

    def each(lo, hi, f):
        lax.fori_loop(lo, hi, lambda q, x: (f(plane(q)), x)[1], 0)

    load = pltpu.make_async_copy(particles, held.at[me], local_sem)
    load.start()
    barrier = pltpu.get_barrier_semaphore()

    def greet(way):
        pl.semaphore_signal(barrier, inc=1, device_id={"dom": target[way]}, device_id_type=MESH)

    greet("core")
    greet("side")
    pl.when(has_up)(lambda: greet("up"))
    pl.when(has_down)(lambda: greet("down"))

    m = rows.shape[1]
    square = (m, m)
    diagonal = lax.broadcasted_iota(jnp.int32, square, 0) == lax.broadcasted_iota(jnp.int32, square, 1)
    local = (index[...] - me * own_rows).astype(jnp.float32)
    wanted = jnp.sum(jnp.where(diagonal, jnp.broadcast_to(local, square), 0.0), axis=1, keepdims=True)
    pick = lax.broadcasted_iota(jnp.int32, (m, own_rows), 1).astype(jnp.float32) == wanted
    targets = jnp.sum(jnp.where(pick, jnp.broadcast_to(labels[...].astype(jnp.float32), pick.shape), 0.0),
                      axis=1, keepdims=True)
    pick_b = pick.astype(jnp.float32).astype(jnp.bfloat16)
    rows[me, :, pl.ds(d, 128)] = jnp.broadcast_to(targets, (m, 128)).astype(jnp.bfloat16)
    for t in range(0, d, TILE):
        rows[me, :, pl.ds(t, TILE)] = jnp.dot(
            pick_b, dataset[:, pl.ds(t, TILE)], preferred_element_type=jnp.float32).astype(jnp.bfloat16)

    pl.semaphore_wait(barrier, 2 + has_up.astype(jnp.int32) + has_down.astype(jnp.int32))

    own(row_stream, True)
    own_cross(row_stream, True)
    each(1, planes, lambda p: relay(row_stream, p, True))
    load.wait()
    own(part_stream, True)
    each(0, planes, lambda p: finish_side(row_stream, p, True))
    own_cross(part_stream, True)
    each(0, planes, lambda p: finish_core(row_stream, p))

    drive[...] = jnp.zeros_like(drive)
    pull[...] = jnp.zeros_like(pull)
    rowsum[...] = jnp.zeros_like(rowsum)
    labels_in = rows[:, :, pl.ds(d, 128)].reshape(batch, 128).astype(jnp.float32)
    target_row[...] = jnp.transpose(labels_in)[0:8, :]
    own_f = held[me].astype(jnp.float32)
    own_sq[...] = jnp.broadcast_to(jnp.sum(own_f * own_f, axis=1, keepdims=True), own_sq.shape)

    def columns(t):
        return pl.ds(pl.multiple_of(t * TILE, TILE), TILE)

    def absorb(p):
        first = p * 4

        def measure(t, sums):
            logits, cross, sq = sums
            part = held[pl.ds(first, 4), :, columns(t)].reshape(group, TILE)
            feat = rows[:, :, columns(t)].reshape(batch, TILE)
            mine = held[me, :, columns(t)]
            nt = (((1,), (1,)), ((), ()))
            logits += lax.dot_general(part, feat, nt, preferred_element_type=jnp.float32)
            cross += lax.dot_general(mine, part, nt, preferred_element_type=jnp.float32)
            part_f = part.astype(jnp.float32)
            part_f = part_f * part_f
            for i in range(0, TILE, 128):
                sq += part_f[:, i:i + 128]
            return logits, cross, sq

        logits, cross, sq = lax.fori_loop(0, d // TILE, measure, (
            jnp.zeros((group, batch), jnp.float32), jnp.zeros((particles.shape[0], group), jnp.float32),
            jnp.zeros((group, 128), jnp.float32)))
        misfit = (target_row[0:1, :] - jax.nn.sigmoid(logits)).astype(jnp.bfloat16)
        sq = jnp.transpose(jnp.broadcast_to(jnp.sum(sq, axis=1, keepdims=True), (group, 128)))[0:1, :]
        dist = own_sq[:, 0:1] + sq - 2.0 * cross
        weight = jnp.exp(-dist * inv_scale)
        rowsum[...] += jnp.broadcast_to(jnp.sum(weight, axis=1, keepdims=True), rowsum.shape)
        weight_b = weight.astype(jnp.bfloat16)

        @pl.loop(0, d // TILE)
        def _(t):
            part = held[pl.ds(first, 4), :, columns(t)].reshape(group, TILE)
            feat = rows[:, :, columns(t)].reshape(batch, TILE)
            pulled = jnp.dot(misfit, feat, preferred_element_type=jnp.float32)
            score = (ratio * pulled - prior_precision * part.astype(jnp.float32)).astype(jnp.bfloat16)
            drive[:, columns(t)] += jnp.dot(weight_b, score, preferred_element_type=jnp.float32)
            pull[:, columns(t)] += jnp.dot(weight_b, part, preferred_element_type=jnp.float32)

    def step(q, done):
        p = plane(q)
        ready = jnp.minimum(within(distance(q) + 1), planes)
        each(done, ready, lambda r: relay(part_stream, r, True))
        finish_side(part_stream, p, True)
        finish_core(part_stream, p)
        absorb(p)
        return ready

    lax.fori_loop(0, planes, step, jnp.int32(1))

    drive_out[...] = drive[...] / total
    spread_out[...] = (held[me].astype(jnp.float32) * rowsum[:, 0:1] - pull[...]) / total

    for st in (row_stream, part_stream):
        own(st, False)
        own_cross(st, False)
        each(1, planes, functools.partial(relay, st, go=False))
        each(0, planes, functools.partial(finish_side, st, go=False))


def per_device(particles, dataset, labels, batch_index):
    n = lax.axis_size("dom")
    k, d = particles.shape
    m = batch_index.shape[0]
    vmem = pl.BlockSpec(memory_space=pltpu.VMEM)
    sems = [pltpu.SemaphoreType.DMA((2, n))] * 10
    out = jax.ShapeDtypeStruct((k, d), jnp.float32)
    return pl.pallas_call(
        functools.partial(kernel, n),
        out_shape=(out, out),
        in_specs=[pl.BlockSpec(memory_space=pl.ANY), vmem, vmem, vmem],
        out_specs=(vmem, vmem),
        scratch_shapes=[
            pltpu.VMEM((n, k, d), jnp.bfloat16),
            pltpu.VMEM((n, m, d + 128), jnp.bfloat16),
            pltpu.VMEM((k, d), jnp.float32),
            pltpu.VMEM((k, d), jnp.float32),
            pltpu.VMEM((k, 128), jnp.float32),
            pltpu.VMEM((8, n * m), jnp.float32),
            pltpu.VMEM((k, 128), jnp.float32),
            pltpu.SemaphoreType.DMA,
        ] + sems,
        compiler_params=pltpu.CompilerParams(
            collective_id=0, has_side_effects=True, vmem_limit_bytes=56 * 1024 * 1024),
    )(particles, dataset, labels[None, :], batch_index[None, :])


def solution(mesh):
    whole = P(("groups", "dom"), None)
    return jax.shard_map(
        per_device,
        mesh=mesh,
        in_specs=(whole, whole, P(("groups", "dom")), P(("groups", "dom"))),
        out_specs=(whole, whole),
        check_vma=False,
    )
```

```python
import functools

import jax
import jax.numpy as jnp
from jax import lax
from jax.experimental import pallas as pl
from jax.experimental.pallas import tpu as pltpu
from jax.sharding import PartitionSpec as P

prior_precision = 1.0
MESH = pl.DeviceIdType.MESH
CROSS = 512
PIECES = 1
TILE = 512
MEASURE = 4096
APPLY = 4096


def cut(d, extra):
    step = -(-(d - CROSS) // (PIECES * TILE)) * TILE
    starts = list(range(0, d - CROSS, step))
    return [(a, min(step, d - CROSS - a)) for a in starts] + [(d - CROSS, CROSS + extra)]


class Stream:
    def __init__(self, buf, splits, recv, up, down, side, core):
        self.buf, self.splits, self.recv = buf, splits, recv
        self.sems = {"up": up, "down": down, "side": side, "core": core}


def kernel(n, particles, dataset, labels, index, drive_out, spread_out,
           held, rows, drive, pull, rowsum, target_row, own_sq, data, local_sem, data_sem, *sems):
    planes = n // 4
    d = particles.shape[1]
    batch = rows.shape[0] * rows.shape[1]
    group = 4 * particles.shape[0]
    own_rows = dataset.shape[0]
    ratio = float(own_rows) / float(rows.shape[1])
    inv_scale = 1.0 / (0.25 * d)
    total = float(particles.shape[0] * n)

    me = lax.axis_index("dom")
    core = me % 2
    y = (me // 2) % 2
    z = me // 4
    target = {"up": me + 4, "down": me - 4, "side": me + 2 - 4 * y, "core": me + 1 - 2 * core}
    has_up, has_down = z < planes - 1, z > 0
    row_stream = Stream(rows, cut(d, 128), *sems[:5])
    part_stream = Stream(held, cut(d, 0), *sems[5:])
    last = len(row_stream.splits) - 1
    main = range(last)

    def block_of(p, yy, cc):
        return (p * 2 + yy) * 2 + cc

    def copy(st, k, b, way):
        view = st.buf.at[b, :, pl.ds(*st.splits[k])]
        return pltpu.make_async_remote_copy(
            src_ref=view, dst_ref=view, send_sem=st.sems[way].at[k, b], recv_sem=st.recv.at[k, b],
            device_id={"dom": target[way]}, device_id_type=MESH)

    def send(st, k, b, way, go):
        c = copy(st, k, b, way)
        c.start() if go else c.wait_send()

    def arrived(st, k, b):
        copy(st, k, b, "core").wait_recv()

    def own_column(st, way, go):
        for k in range(last + 1):
            send(st, k, me, way, go)

    def own_side(st, go):
        for k in main:
            send(st, k, me, "side", go)

    def own_core(st, go):
        for k in range(last + 1):
            send(st, k, me, "core", go)

    def own_cross(st, go):
        b = target["side"]
        if go:
            arrived(st, last, b)

        @pl.when(has_up)
        def _():
            send(st, last, b, "up", go)

        @pl.when(has_down)
        def _():
            send(st, last, b, "down", go)

        send(st, last, b, "core", go)

    def relay(st, s, go):
        def one(valid, p, onward, way, k, across):
            @pl.when(valid)
            def _():
                b = block_of(p, 1 - y if across else y, core)
                if go:
                    arrived(st, k, b)

                @pl.when(onward)
                def _():
                    send(st, k, b, way, go)

                if k < last:
                    send(st, k, b, "side", go)
                send(st, k, b, "core", go)

        for k, across in [(k, False) for k in range(last + 1)] + [(last, True)]:
            one(z - s >= 0, z - s, has_up, "up", k, across)
            one(z + s < planes, z + s, has_down, "down", k, across)

    def side_piece(st, k, p, go):
        b = block_of(p, 1 - y, core)
        if go:
            arrived(st, k, b)
        send(st, k, b, "core", go)

    def finish_side(st, p, go):
        for k in main:
            side_piece(st, k, p, go)

    def core_piece(st, k, p):
        for yy in (0, 1):
            arrived(st, k, block_of(p, yy, 1 - core))

    def finish_core(st, p):
        for k in range(last + 1):
            core_piece(st, k, p)

    near = jnp.minimum(z, planes - 1 - z)
    outward = jnp.where(z <= planes - 1 - z, 1, -1)

    def distance(q):
        return jnp.where(q <= 2 * near, (q + 1) // 2, q - near)

    def plane(q):
        two_sided = jnp.where(q % 2 == 1, -1, 1)
        return z + jnp.where(q <= 2 * near, two_sided, outward) * distance(q)

    reach = jnp.maximum(z, planes - 1 - z)

    def each(lo, hi, f):
        lax.fori_loop(lo, hi, lambda q, x: (f(plane(q)), x)[1], 0)

    load = pltpu.make_async_copy(particles, held.at[me], local_sem)
    fetch = pltpu.make_async_copy(dataset, data, data_sem)
    fetch.start()
    load.start()
    barrier = pltpu.get_barrier_semaphore()

    def greet(way):
        pl.semaphore_signal(barrier, inc=1, device_id={"dom": target[way]}, device_id_type=MESH)

    greet("core")
    greet("side")
    pl.when(has_up)(lambda: greet("up"))
    pl.when(has_down)(lambda: greet("down"))

    m = rows.shape[1]
    square = (m, m)
    diagonal = lax.broadcasted_iota(jnp.int32, square, 0) == lax.broadcasted_iota(jnp.int32, square, 1)
    local = (index[...] - me * own_rows).astype(jnp.float32)
    wanted = jnp.sum(jnp.where(diagonal, jnp.broadcast_to(local, square), 0.0), axis=1, keepdims=True)
    pick = lax.broadcasted_iota(jnp.int32, (m, own_rows), 1).astype(jnp.float32) == wanted
    targets = jnp.sum(jnp.where(pick, jnp.broadcast_to(labels[...].astype(jnp.float32), pick.shape), 0.0),
                      axis=1, keepdims=True)
    pick_b = pick.astype(jnp.float32).astype(jnp.bfloat16)
    rows[me, :, pl.ds(d, 128)] = jnp.broadcast_to(targets, (m, 128)).astype(jnp.bfloat16)
    fetch.wait()
    for t in range(0, d, TILE):
        rows[me, :, pl.ds(t, TILE)] = jnp.dot(
            pick_b, data[:, pl.ds(t, TILE)], preferred_element_type=jnp.float32).astype(jnp.bfloat16)

    pl.semaphore_wait(barrier, 2 + has_up.astype(jnp.int32) + has_down.astype(jnp.int32))

    def column(st, cond, way, go):
        pl.when(cond)(lambda: own_column(st, way, go))

    send(row_stream, last, me, "side", True)
    own_side(row_stream, True)
    column(row_stream, has_up, "up", True)
    column(row_stream, has_down, "down", True)
    own_core(row_stream, True)
    load.wait()
    send(part_stream, last, me, "side", True)
    own_core(part_stream, True)
    own_cross(row_stream, True)
    column(part_stream, z == 0, "up", True)
    column(part_stream, z == planes - 1, "down", True)

    def relay_rows(s, x):
        relay(row_stream, s, True)
        column(part_stream, jnp.logical_and(s == z, has_up), "up", True)
        column(part_stream, jnp.logical_and(s == planes - 1 - z, has_down), "down", True)
        return x

    lax.fori_loop(1, reach + 1, relay_rows, 0)
    own_side(part_stream, True)
    each(0, planes, lambda p: finish_side(row_stream, p, True))
    own_cross(part_stream, True)
    each(0, planes, lambda p: finish_core(row_stream, p))

    drive[...] = jnp.zeros_like(drive)
    pull[...] = jnp.zeros_like(pull)
    rowsum[...] = jnp.zeros_like(rowsum)
    labels_in = rows[:, :, pl.ds(d, 128)].reshape(batch, 128).astype(jnp.float32)
    target_row[...] = jnp.transpose(labels_in)[0:8, :]
    own_f = held[me].astype(jnp.float32)
    own_sq[...] = jnp.broadcast_to(jnp.sum(own_f * own_f, axis=1, keepdims=True), own_sq.shape)

    def columns(t, width):
        return pl.ds(pl.multiple_of(t * width, width), width)

    def absorb(p):
        first = p * 4

        def measure(t, sums):
            logits, cross, sq = sums
            part = held[pl.ds(first, 4), :, columns(t, MEASURE)].reshape(group, MEASURE)
            feat = rows[:, :, columns(t, MEASURE)].reshape(batch, MEASURE)
            mine = held[me, :, columns(t, MEASURE)]
            nt = (((1,), (1,)), ((), ()))
            logits += lax.dot_general(part, feat, nt, preferred_element_type=jnp.float32)
            cross += lax.dot_general(mine, part, nt, preferred_element_type=jnp.float32)
            part_f = part.astype(jnp.float32)
            part_f = part_f * part_f
            for i in range(0, MEASURE, 128):
                sq += part_f[:, i:i + 128]
            return logits, cross, sq

        sums = (jnp.zeros((group, batch), jnp.float32), jnp.zeros((particles.shape[0], group), jnp.float32),
                jnp.zeros((group, 128), jnp.float32))
        finish_side(part_stream, p, True)
        finish_core(part_stream, p)
        logits, cross, sq = lax.fori_loop(0, d // MEASURE, measure, sums)
        misfit = (target_row[0:1, :] - jax.nn.sigmoid(logits)).astype(jnp.bfloat16)
        sq = jnp.transpose(jnp.broadcast_to(jnp.sum(sq, axis=1, keepdims=True), (group, 128)))[0:1, :]
        dist = own_sq[:, 0:1] + sq - 2.0 * cross
        weight = jnp.exp(-dist * inv_scale)
        rowsum[...] += jnp.broadcast_to(jnp.sum(weight, axis=1, keepdims=True), rowsum.shape)
        weight_b = weight.astype(jnp.bfloat16)

        @pl.loop(0, d // APPLY)
        def _(t):
            part = held[pl.ds(first, 4), :, columns(t, APPLY)].reshape(group, APPLY)
            feat = rows[:, :, columns(t, APPLY)].reshape(batch, APPLY)
            pulled = jnp.dot(misfit, feat, preferred_element_type=jnp.float32)
            score = (ratio * pulled - prior_precision * part.astype(jnp.float32)).astype(jnp.bfloat16)
            drive[:, columns(t, APPLY)] += jnp.dot(weight_b, score, preferred_element_type=jnp.float32)
            pull[:, columns(t, APPLY)] += jnp.dot(weight_b, part, preferred_element_type=jnp.float32)

    def pass_on(lo, hi, go):
        lax.fori_loop(lo, hi, lambda s, x: (relay(part_stream, s, go), x)[1], 0)

    def step(q, done):
        p = plane(q)
        ready = jnp.minimum(distance(q) + 1, reach) + 1
        pass_on(done, ready, True)
        absorb(p)
        return ready

    def settle(st, until):
        send(st, last, me, "side", False)
        own_side(st, False)
        own_core(st, False)
        column(st, has_up, "up", False)
        column(st, has_down, "down", False)
        own_cross(st, False)
        each(0, until, functools.partial(finish_side, st, go=False))

    done = lax.fori_loop(0, planes - 1, step, jnp.int32(1))
    settle(row_stream, planes)
    lax.fori_loop(1, reach + 1, lambda s, x: (relay(row_stream, s, False), x)[1], 0)
    settle(part_stream, planes - 1)
    step(planes - 1, done)

    drive_out[...] = drive[...] / total
    spread_out[...] = (held[me].astype(jnp.float32) * rowsum[:, 0:1] - pull[...]) / total

    finish_side(part_stream, plane(planes - 1), False)
    pass_on(1, reach + 1, False)


def per_device(particles, dataset, labels, batch_index):
    n = lax.axis_size("dom")
    k, d = particles.shape
    m = batch_index.shape[0]
    vmem = pl.BlockSpec(memory_space=pltpu.VMEM)
    sems = [pltpu.SemaphoreType.DMA((len(cut(d, 0)), n))] * 10

    out = jax.ShapeDtypeStruct((k, d), jnp.float32)
    return pl.pallas_call(
        functools.partial(kernel, n),
        out_shape=(out, out),
        in_specs=[pl.BlockSpec(memory_space=pltpu.HBM)] * 2 + [vmem] * 2,
        out_specs=(vmem, vmem),
        scratch_shapes=[
            pltpu.VMEM((n, k, d), jnp.bfloat16),
            pltpu.VMEM((n, m, d + 128), jnp.bfloat16),
            pltpu.VMEM((k, d), jnp.float32),
            pltpu.VMEM((k, d), jnp.float32),
            pltpu.VMEM((k, 128), jnp.float32),
            pltpu.VMEM((8, n * m), jnp.float32),
            pltpu.VMEM((k, 128), jnp.float32),
            pltpu.VMEM(dataset.shape, jnp.bfloat16),
            pltpu.SemaphoreType.DMA,
            pltpu.SemaphoreType.DMA,
        ] + sems,
        compiler_params=pltpu.CompilerParams(
            collective_id=0, has_side_effects=True, vmem_limit_bytes=56 * 1024 * 1024),
    )(particles, dataset, labels[None, :], batch_index[None, :])


def solution(mesh):
    whole = P(("groups", "dom"), None)
    return jax.shard_map(
        per_device,
        mesh=mesh,
        in_specs=(whole, whole, P(("groups", "dom")), P(("groups", "dom"))),
        out_specs=(whole, whole),
        check_vma=False,
    )
```

```python
import functools

import jax
import jax.numpy as jnp
from jax import lax
from jax.experimental import pallas as pl
from jax.experimental.pallas import tpu as pltpu
from jax.sharding import PartitionSpec as P

prior_precision = 1.0
MESH = pl.DeviceIdType.MESH
CROSS = 512
PIECES = 2
TILE = 512


def cut(d, extra):
    step = -(-(d - CROSS) // (PIECES * 128)) * 128
    starts = list(range(0, d - CROSS, step))
    return [(a, min(step, d - CROSS - a)) for a in starts] + [(d - CROSS, CROSS + extra)]


class Stream:
    def __init__(self, buf, splits, recv, up, down, side, core):
        self.buf, self.splits, self.recv = buf, splits, recv
        self.sems = {"up": up, "down": down, "side": side, "core": core}


def kernel(n, particles, dataset, labels, index, drive_out, spread_out,
           held, rows, drive, pull, rowsum, target_row, own_sq, data, local_sem, data_sem, *sems):
    planes = n // 4
    d = particles.shape[1]
    batch = rows.shape[0] * rows.shape[1]
    group = 4 * particles.shape[0]
    own_rows = dataset.shape[0]
    ratio = float(own_rows) / float(rows.shape[1])
    inv_scale = 1.0 / (0.25 * d)
    total = float(particles.shape[0] * n)

    me = lax.axis_index("dom")
    core = me % 2
    y = (me // 2) % 2
    z = me // 4
    target = {"up": me + 4, "down": me - 4, "side": me + 2 - 4 * y, "core": me + 1 - 2 * core}
    has_up, has_down = z < planes - 1, z > 0
    row_stream = Stream(rows, cut(d, 128), *sems[:5])
    part_stream = Stream(held, cut(d, 0), *sems[5:])
    last = len(row_stream.splits) - 1
    main = range(last)

    def block_of(p, yy, cc):
        return (p * 2 + yy) * 2 + cc

    def copy(st, k, b, way):
        view = st.buf.at[b, :, pl.ds(*st.splits[k])]
        return pltpu.make_async_remote_copy(
            src_ref=view, dst_ref=view, send_sem=st.sems[way].at[k, b], recv_sem=st.recv.at[k, b],
            device_id={"dom": target[way]}, device_id_type=MESH)

    def send(st, k, b, way, go):
        c = copy(st, k, b, way)
        c.start() if go else c.wait_send()

    def arrived(st, k, b):
        copy(st, k, b, "core").wait_recv()

    def own_column(st, way, go):
        for k in range(last + 1):
            send(st, k, me, way, go)

    def own_side(st, go):
        for k in main:
            send(st, k, me, "side", go)

    def own_core(st, go):
        for k in range(last + 1):
            send(st, k, me, "core", go)

    def own_cross(st, go):
        b = target["side"]
        if go:
            arrived(st, last, b)

        @pl.when(has_up)
        def _():
            send(st, last, b, "up", go)

        @pl.when(has_down)
        def _():
            send(st, last, b, "down", go)

        send(st, last, b, "core", go)

    def relay(st, s, go):
        def one(valid, p, onward, way, k, across):
            @pl.when(valid)
            def _():
                b = block_of(p, 1 - y if across else y, core)
                if go:
                    arrived(st, k, b)

                @pl.when(onward)
                def _():
                    send(st, k, b, way, go)

                if k < last:
                    send(st, k, b, "side", go)
                send(st, k, b, "core", go)

        for k, across in [(k, False) for k in range(last + 1)] + [(last, True)]:
            one(z - s >= 0, z - s, has_up, "up", k, across)
            one(z + s < planes, z + s, has_down, "down", k, across)

    def side_piece(st, k, p, go):
        b = block_of(p, 1 - y, core)
        if go:
            arrived(st, k, b)
        send(st, k, b, "core", go)

    def finish_side(st, p, go):
        for k in main:
            side_piece(st, k, p, go)

    def core_piece(st, k, p):
        for yy in (0, 1):
            arrived(st, k, block_of(p, yy, 1 - core))

    def finish_core(st, p):
        for k in range(last + 1):
            core_piece(st, k, p)

    near = jnp.minimum(z, planes - 1 - z)
    outward = jnp.where(z <= planes - 1 - z, 1, -1)

    def distance(q):
        return jnp.where(q <= 2 * near, (q + 1) // 2, q - near)

    def plane(q):
        two_sided = jnp.where(q % 2 == 1, -1, 1)
        return z + jnp.where(q <= 2 * near, two_sided, outward) * distance(q)

    reach = jnp.maximum(z, planes - 1 - z)

    def each(lo, hi, f):
        lax.fori_loop(lo, hi, lambda q, x: (f(plane(q)), x)[1], 0)

    load = pltpu.make_async_copy(particles, held.at[me], local_sem)
    fetch = pltpu.make_async_copy(dataset, data, data_sem)
    fetch.start()
    load.start()
    barrier = pltpu.get_barrier_semaphore()

    def greet(way):
        pl.semaphore_signal(barrier, inc=1, device_id={"dom": target[way]}, device_id_type=MESH)

    greet("core")
    greet("side")
    pl.when(has_up)(lambda: greet("up"))
    pl.when(has_down)(lambda: greet("down"))

    m = rows.shape[1]
    square = (m, m)
    diagonal = lax.broadcasted_iota(jnp.int32, square, 0) == lax.broadcasted_iota(jnp.int32, square, 1)
    local = (index[...] - me * own_rows).astype(jnp.float32)
    wanted = jnp.sum(jnp.where(diagonal, jnp.broadcast_to(local, square), 0.0), axis=1, keepdims=True)
    pick = lax.broadcasted_iota(jnp.int32, (m, own_rows), 1).astype(jnp.float32) == wanted
    targets = jnp.sum(jnp.where(pick, jnp.broadcast_to(labels[...].astype(jnp.float32), pick.shape), 0.0),
                      axis=1, keepdims=True)
    pick_b = pick.astype(jnp.float32).astype(jnp.bfloat16)
    rows[me, :, pl.ds(d, 128)] = jnp.broadcast_to(targets, (m, 128)).astype(jnp.bfloat16)
    fetch.wait()
    for t in range(0, d, TILE):
        rows[me, :, pl.ds(t, TILE)] = jnp.dot(
            pick_b, data[:, pl.ds(t, TILE)], preferred_element_type=jnp.float32).astype(jnp.bfloat16)

    pl.semaphore_wait(barrier, 2 + has_up.astype(jnp.int32) + has_down.astype(jnp.int32))

    def column(st, cond, way, go):
        pl.when(cond)(lambda: own_column(st, way, go))

    send(row_stream, last, me, "side", True)
    own_side(row_stream, True)
    column(row_stream, has_up, "up", True)
    column(row_stream, has_down, "down", True)
    own_core(row_stream, True)
    load.wait()
    send(part_stream, last, me, "side", True)
    own_core(part_stream, True)
    own_cross(row_stream, True)
    column(part_stream, z == 0, "up", True)
    column(part_stream, z == planes - 1, "down", True)

    def relay_rows(s, x):
        relay(row_stream, s, True)
        column(part_stream, jnp.logical_and(s == z, has_up), "up", True)
        column(part_stream, jnp.logical_and(s == planes - 1 - z, has_down), "down", True)
        return x

    lax.fori_loop(1, reach + 1, relay_rows, 0)
    own_side(part_stream, True)
    each(0, planes, lambda p: finish_side(row_stream, p, True))
    own_cross(part_stream, True)
    each(0, planes, lambda p: finish_core(row_stream, p))

    drive[...] = jnp.zeros_like(drive)
    pull[...] = jnp.zeros_like(pull)
    rowsum[...] = jnp.zeros_like(rowsum)
    labels_in = rows[:, :, pl.ds(d, 128)].reshape(batch, 128).astype(jnp.float32)
    target_row[...] = jnp.transpose(labels_in)[0:8, :]
    own_f = held[me].astype(jnp.float32)
    own_sq[...] = jnp.broadcast_to(jnp.sum(own_f * own_f, axis=1, keepdims=True), own_sq.shape)

    def absorb(p):
        first = p * 4

        finish_side(part_stream, p, True)
        finish_core(part_stream, p)
        part = held[pl.ds(first, 4)].reshape(group, d)
        feat = rows[:, :, pl.ds(0, d)].reshape(batch, d)
        nt = (((1,), (1,)), ((), ()))
        logits = lax.dot_general(part, feat, nt, preferred_element_type=jnp.float32)
        cross = lax.dot_general(held[me], part, nt, preferred_element_type=jnp.float32)
        part_f = part.astype(jnp.float32)
        sq = jnp.sum(part_f * part_f, axis=1, keepdims=True)
        misfit = (target_row[0:1, :] - jax.nn.sigmoid(logits)).astype(jnp.bfloat16)
        sq = jnp.transpose(jnp.broadcast_to(sq, (group, 128)))[0:1, :]
        dist = own_sq[:, 0:1] + sq - 2.0 * cross
        weight = jnp.exp(-dist * inv_scale)
        rowsum[...] += jnp.broadcast_to(jnp.sum(weight, axis=1, keepdims=True), rowsum.shape)
        weight_b = weight.astype(jnp.bfloat16)

        pulled = jnp.dot(misfit, feat, preferred_element_type=jnp.float32)
        score = (ratio * pulled - prior_precision * part_f).astype(jnp.bfloat16)
        drive[...] += jnp.dot(weight_b, score, preferred_element_type=jnp.float32)
        pull[...] += jnp.dot(weight_b, part, preferred_element_type=jnp.float32)

    def pass_on(lo, hi, go):
        lax.fori_loop(lo, hi, lambda s, x: (relay(part_stream, s, go), x)[1], 0)

    def step(q, done):
        p = plane(q)
        ready = jnp.minimum(distance(q) + 1, reach) + 1
        pass_on(done, ready, True)
        absorb(p)
        return ready

    def settle(st, until):
        send(st, last, me, "side", False)
        own_side(st, False)
        own_core(st, False)
        column(st, has_up, "up", False)
        column(st, has_down, "down", False)
        own_cross(st, False)
        each(0, until, functools.partial(finish_side, st, go=False))

    done = lax.fori_loop(0, planes - 1, step, jnp.int32(1))
    settle(row_stream, planes)
    lax.fori_loop(1, reach + 1, lambda s, x: (relay(row_stream, s, False), x)[1], 0)
    settle(part_stream, planes - 1)
    step(planes - 1, done)

    drive_out[...] = drive[...] / total
    spread_out[...] = (held[me].astype(jnp.float32) * rowsum[:, 0:1] - pull[...]) / total

    finish_side(part_stream, plane(planes - 1), False)
    pass_on(1, reach + 1, False)


def per_device(particles, dataset, labels, batch_index):
    n = lax.axis_size("dom")
    k, d = particles.shape
    m = batch_index.shape[0]
    vmem = pl.BlockSpec(memory_space=pltpu.VMEM)
    sems = [pltpu.SemaphoreType.DMA((len(cut(d, 0)), n))] * 10

    out = jax.ShapeDtypeStruct((k, d), jnp.float32)
    return pl.pallas_call(
        functools.partial(kernel, n),
        out_shape=(out, out),
        in_specs=[pl.BlockSpec(memory_space=pltpu.HBM)] * 2 + [vmem] * 2,
        out_specs=(vmem, vmem),
        scratch_shapes=[
            pltpu.VMEM((n, k, d), jnp.bfloat16),
            pltpu.VMEM((n, m, d + 128), jnp.bfloat16),
            pltpu.VMEM((k, d), jnp.float32),
            pltpu.VMEM((k, d), jnp.float32),
            pltpu.VMEM((k, 128), jnp.float32),
            pltpu.VMEM((8, n * m), jnp.float32),
            pltpu.VMEM((k, 128), jnp.float32),
            pltpu.VMEM(dataset.shape, jnp.bfloat16),
            pltpu.SemaphoreType.DMA,
            pltpu.SemaphoreType.DMA,
        ] + sems,
        compiler_params=pltpu.CompilerParams(
            collective_id=0, has_side_effects=True, vmem_limit_bytes=56 * 1024 * 1024),
    )(particles, dataset, labels[None, :], batch_index[None, :])


def solution(mesh):
    whole = P(("groups", "dom"), None)
    return jax.shard_map(
        per_device,
        mesh=mesh,
        in_specs=(whole, whole, P(("groups", "dom")), P(("groups", "dom"))),
        out_specs=(whole, whole),
        check_vma=False,
    )
```

```python
import functools

import jax
import jax.numpy as jnp
from jax import lax
from jax.experimental import pallas as pl
from jax.experimental.pallas import tpu as pltpu
from jax.sharding import PartitionSpec as P

prior_precision = 1.0
MESH = pl.DeviceIdType.MESH
CROSS = 512
PIECES = 2
TILE = 512


def cut(d, extra):
    step = -(-(d - CROSS) // (PIECES * 128)) * 128
    starts = list(range(0, d - CROSS, step))
    return [(a, min(step, d - CROSS - a)) for a in starts] + [(d - CROSS, CROSS + extra)]


class Stream:
    def __init__(self, buf, splits, recv, up, down, side, core):
        self.buf, self.splits, self.recv = buf, splits, recv
        self.sems = {"up": up, "down": down, "side": side, "core": core}


def kernel(n, particles, dataset, labels, index, drive_out, spread_out,
           held, rows, drive, pull, rowsum, target_row, own_sq, data, local_sem, data_sem, *sems):
    planes = n // 4
    d = particles.shape[1]
    batch = rows.shape[0] * rows.shape[1]
    group = 4 * particles.shape[0]
    own_rows = dataset.shape[0]
    ratio = float(own_rows) / float(rows.shape[1])
    inv_scale = 1.0 / (0.25 * d)
    total = float(particles.shape[0] * n)

    me = lax.axis_index("dom")
    core = me % 2
    y = (me // 2) % 2
    z = me // 4
    target = {"up": me + 4, "down": me - 4, "side": me + 2 - 4 * y, "core": me + 1 - 2 * core}
    has_up, has_down = z < planes - 1, z > 0
    row_stream = Stream(rows, cut(d, 128), *sems[:5])
    part_stream = Stream(held, cut(d, 0), *sems[5:])
    last = len(row_stream.splits) - 1
    main = range(last)

    def block_of(p, yy, cc):
        return (p * 2 + yy) * 2 + cc

    def copy(st, k, b, way):
        view = st.buf.at[b, :, pl.ds(*st.splits[k])]
        return pltpu.make_async_remote_copy(
            src_ref=view, dst_ref=view, send_sem=st.sems[way].at[k, b], recv_sem=st.recv.at[k, b],
            device_id={"dom": target[way]}, device_id_type=MESH)

    def send(st, k, b, way, go):
        c = copy(st, k, b, way)
        c.start() if go else c.wait_send()

    def arrived(st, k, b):
        copy(st, k, b, "core").wait_recv()

    def own_column(st, way, go):
        for k in range(last + 1):
            send(st, k, me, way, go)

    def own_side(st, go):
        for k in main:
            send(st, k, me, "side", go)

    def own_core(st, go):
        for k in range(last + 1):
            send(st, k, me, "core", go)

    def own_cross(st, go):
        b = target["side"]
        if go:
            arrived(st, last, b)

        @pl.when(has_up)
        def _():
            send(st, last, b, "up", go)

        @pl.when(has_down)
        def _():
            send(st, last, b, "down", go)

        send(st, last, b, "core", go)

    def relay(st, s, go):
        def one(valid, p, onward, way, k, across):
            @pl.when(valid)
            def _():
                b = block_of(p, 1 - y if across else y, core)
                if go:
                    arrived(st, k, b)

                @pl.when(onward)
                def _():
                    send(st, k, b, way, go)

                if k < last:
                    send(st, k, b, "side", go)
                send(st, k, b, "core", go)

        for k, across in [(k, False) for k in range(last + 1)] + [(last, True)]:
            one(z - s >= 0, z - s, has_up, "up", k, across)
            one(z + s < planes, z + s, has_down, "down", k, across)

    def side_piece(st, k, p, go):
        b = block_of(p, 1 - y, core)
        if go:
            arrived(st, k, b)
        send(st, k, b, "core", go)

    def finish_side(st, p, go):
        for k in main:
            side_piece(st, k, p, go)

    def core_piece(st, k, p):
        for yy in (0, 1):
            arrived(st, k, block_of(p, yy, 1 - core))

    def finish_core(st, p):
        for k in range(last + 1):
            core_piece(st, k, p)

    near = jnp.minimum(z, planes - 1 - z)
    outward = jnp.where(z <= planes - 1 - z, 1, -1)

    def distance(q):
        return jnp.where(q <= 2 * near, (q + 1) // 2, q - near)

    def plane(q):
        two_sided = jnp.where(q % 2 == 1, -1, 1)
        return z + jnp.where(q <= 2 * near, two_sided, outward) * distance(q)

    reach = jnp.maximum(z, planes - 1 - z)

    def each(lo, hi, f):
        lax.fori_loop(lo, hi, lambda q, x: (f(plane(q)), x)[1], 0)

    load = pltpu.make_async_copy(particles, held.at[me], local_sem)
    fetch = pltpu.make_async_copy(dataset, data, data_sem)
    fetch.start()
    load.start()
    barrier = pltpu.get_barrier_semaphore()

    def greet(way):
        pl.semaphore_signal(barrier, inc=1, device_id={"dom": target[way]}, device_id_type=MESH)

    greet("core")
    greet("side")
    pl.when(has_up)(lambda: greet("up"))
    pl.when(has_down)(lambda: greet("down"))

    m = rows.shape[1]
    square = (m, m)
    diagonal = lax.broadcasted_iota(jnp.int32, square, 0) == lax.broadcasted_iota(jnp.int32, square, 1)
    local = (index[...] - me * own_rows).astype(jnp.float32)
    wanted = jnp.sum(jnp.where(diagonal, jnp.broadcast_to(local, square), 0.0), axis=1, keepdims=True)
    pick = lax.broadcasted_iota(jnp.int32, (m, own_rows), 1).astype(jnp.float32) == wanted
    targets = jnp.sum(jnp.where(pick, jnp.broadcast_to(labels[...].astype(jnp.float32), pick.shape), 0.0),
                      axis=1, keepdims=True)
    pick_b = pick.astype(jnp.float32).astype(jnp.bfloat16)
    rows[me, :, pl.ds(d, 128)] = jnp.broadcast_to(targets, (m, 128)).astype(jnp.bfloat16)
    fetch.wait()
    for t in range(0, d, TILE):
        rows[me, :, pl.ds(t, TILE)] = jnp.dot(
            pick_b, data[:, pl.ds(t, TILE)], preferred_element_type=jnp.float32).astype(jnp.bfloat16)

    pl.semaphore_wait(barrier, 2 + has_up.astype(jnp.int32) + has_down.astype(jnp.int32))

    def column(st, cond, way, go):
        pl.when(cond)(lambda: own_column(st, way, go))

    send(row_stream, last, me, "side", True)
    own_side(row_stream, True)
    column(row_stream, has_up, "up", True)
    column(row_stream, has_down, "down", True)
    own_core(row_stream, True)
    load.wait()
    send(part_stream, last, me, "side", True)
    own_core(part_stream, True)
    own_cross(row_stream, True)
    column(part_stream, z == 0, "up", True)
    column(part_stream, z == planes - 1, "down", True)

    def relay_rows(s, x):
        relay(row_stream, s, True)
        column(part_stream, jnp.logical_and(s == z, has_up), "up", True)
        column(part_stream, jnp.logical_and(s == planes - 1 - z, has_down), "down", True)
        return x

    lax.fori_loop(1, reach + 1, relay_rows, 0)
    own_side(part_stream, True)
    each(0, planes, lambda p: finish_side(row_stream, p, True))
    own_cross(part_stream, True)
    each(0, planes, lambda p: finish_core(row_stream, p))

    drive[...] = jnp.zeros_like(drive)
    pull[...] = jnp.zeros_like(pull)
    rowsum[...] = jnp.zeros_like(rowsum)
    labels_in = rows[:, :, pl.ds(d, 128)].reshape(batch, 128).astype(jnp.float32)
    target_row[...] = jnp.transpose(labels_in)[0:8, :]
    own_f = held[me].astype(jnp.float32)
    own_sq[...] = jnp.broadcast_to(jnp.sum(own_f * own_f, axis=1, keepdims=True), own_sq.shape)

    def absorb(p):
        first = p * 4

        finish_side(part_stream, p, True)
        finish_core(part_stream, p)
        part = held[pl.ds(first, 4)].reshape(group, d)
        feat = rows[:, :, pl.ds(0, d)].reshape(batch, d)
        nt = (((1,), (1,)), ((), ()))
        logits = lax.dot_general(part, feat, nt, preferred_element_type=jnp.float32)
        cross = lax.dot_general(held[me], part, nt, preferred_element_type=jnp.float32)
        part_f = part.astype(jnp.float32)
        sq = jnp.sum(part_f * part_f, axis=1, keepdims=True)
        misfit = (target_row[0:1, :] - jax.nn.sigmoid(logits)).astype(jnp.bfloat16)
        sq = jnp.transpose(jnp.broadcast_to(sq, (group, 128)))[0:1, :]
        dist = own_sq[:, 0:1] + sq - 2.0 * cross
        weight = jnp.exp(-dist * inv_scale)
        rowsum[...] += jnp.broadcast_to(jnp.sum(weight, axis=1, keepdims=True), rowsum.shape)
        weight_b = weight.astype(jnp.bfloat16)

        pulled = jnp.dot(misfit, feat, preferred_element_type=jnp.float32)
        score = (ratio * pulled - prior_precision * part_f).astype(jnp.bfloat16)
        drive[...] += jnp.dot(weight_b, score, preferred_element_type=jnp.float32)
        pull[...] += jnp.dot(weight_b, part, preferred_element_type=jnp.float32)

    def pass_on(lo, hi, go):
        lax.fori_loop(lo, hi, lambda s, x: (relay(part_stream, s, go), x)[1], 0)

    def step(q, done):
        p = plane(q)
        ready = jnp.minimum(distance(q) + 1, reach) + 1
        pass_on(done, ready, True)
        absorb(p)
        return ready

    def settle(st, until):
        send(st, last, me, "side", False)
        own_side(st, False)
        own_core(st, False)
        column(st, has_up, "up", False)
        column(st, has_down, "down", False)
        own_cross(st, False)
        each(0, until, functools.partial(finish_side, st, go=False))

    done = lax.fori_loop(0, planes - 1, step, jnp.int32(1))
    settle(row_stream, planes)
    lax.fori_loop(1, reach + 1, lambda s, x: (relay(row_stream, s, False), x)[1], 0)
    settle(part_stream, planes - 1)
    step(planes - 1, done)

    drive_out[...] = drive[...] / total
    spread_out[...] = (held[me].astype(jnp.float32) * rowsum[:, 0:1] - pull[...]) / total

    finish_side(part_stream, plane(planes - 1), False)
    pass_on(1, reach + 1, False)


def per_device(particles, dataset, labels, batch_index):
    n = lax.axis_size("dom")
    k, d = particles.shape
    m = batch_index.shape[0]
    vmem = pl.BlockSpec(memory_space=pltpu.VMEM)
    sems = [pltpu.SemaphoreType.DMA((len(cut(d, 0)), n))] * 10

    out = jax.ShapeDtypeStruct((k, d), jnp.float32)
    return pl.pallas_call(
        functools.partial(kernel, n),
        out_shape=(out, out),
        in_specs=[pl.BlockSpec(memory_space=pltpu.HBM)] * 2 + [vmem] * 2,
        out_specs=(vmem, vmem),
        scratch_shapes=[
            pltpu.VMEM((n, k, d), jnp.bfloat16),
            pltpu.VMEM((n, m, d + 128), jnp.bfloat16),
            pltpu.VMEM((k, d), jnp.float32),
            pltpu.VMEM((k, d), jnp.float32),
            pltpu.VMEM((k, 128), jnp.float32),
            pltpu.VMEM((8, n * m), jnp.float32),
            pltpu.VMEM((k, 128), jnp.float32),
            pltpu.VMEM(dataset.shape, jnp.bfloat16),
            pltpu.SemaphoreType.DMA,
            pltpu.SemaphoreType.DMA,
        ] + sems,
        compiler_params=pltpu.CompilerParams(
            collective_id=0, has_side_effects=True, vmem_limit_bytes=53500 * 1024),
    )(particles, dataset, labels[None, :], batch_index[None, :])


def solution(mesh):
    whole = P(("groups", "dom"), None)
    return jax.shard_map(
        per_device,
        mesh=mesh,
        in_specs=(whole, whole, P(("groups", "dom")), P(("groups", "dom"))),
        out_specs=(whole, whole),
        check_vma=False,
    )
```
